32 devices in a mesh: dp: 32 (over z, y, x, core).
Axes of the slice: x: 2, y: 2, z: 4, core: 2. Of those that a mesh axis runs over, the one named last changes fastest.
Arguments:
- act_in: bfloat16 [2048, 7, 7, 2048], P('dp')
- shortcut: bfloat16 [2048, 7, 7, 2048], P('dp')
- labels: int32 [2048], P('dp')
- w_conv: float32 [2048, 2048], replicated
- bn_gamma: float32 [2048], replicated
- bn_beta: float32 [2048], replicated
- w_fc: float32 [2048, 1000], replicated
- fc_bias: float32 [1000], replicated
- vel_conv: float32 [2048, 2048], replicated
- vel_gamma: float32 [2048], replicated
- vel_beta: float32 [2048], replicated
- vel_fc: float32 [2048, 1000], replicated
- vel_bias: float32 [1000], replicated
- learn_rate: float32 [], replicated
Outputs:
- output 1: float32 [2048, 2048], replicated
- output 2: float32 [2048], replicated
- output 3: float32 [2048], replicated
- output 4: float32 [2048, 1000], replicated
- output 5: float32 [1000], replicated
- output 6: float32 [2048, 2048], replicated
- output 7: float32 [2048], replicated
- output 8: float32 [2048], replicated
- output 9: float32 [2048, 1000], replicated
- output 10: float32 [1000], replicated
- output 11: float32 [], replicated
All inputs are finite; a program needn't handle non-finite values.
Results may differ from the reference program's by a relative error of at most 0.00889668.
Values sent between devices are 32-bit elements.
A program may use at most 1 GiB of HBM per device.

```python
import jax
import jax.numpy as jnp
from jax import lax

B_DEV = 64
DP = 32
SIDE = 7
C_MID = 2048
C_OUT = 2048
CLASSES = 1000

BN_EPS = 1e-5
SMOOTHING = 0.1
MOMENTUM = 0.9
TRUST_COEF = 0.001
WEIGHT_DECAY = 5e-5


def setup_inputs(seed: int = 0) -> dict:
    root_key = jax.random.key(seed)
    sub_keys = jax.random.split(root_key, 16)
    global_rows = DP * B_DEV
    step_scale = 2.5
    dev_shift = 0.5 * jax.random.normal(sub_keys[0], (DP, 1, 1, 1, C_MID), jnp.float32)
    act_in = jax.nn.relu(jax.random.normal(sub_keys[1], (DP, B_DEV, SIDE, SIDE, C_MID), jnp.float32) + dev_shift)
    act_in = act_in.reshape(global_rows, SIDE, SIDE, C_MID).astype(jnp.bfloat16)
    shortcut = jax.nn.relu(jax.random.normal(sub_keys[2], (global_rows, SIDE, SIDE, C_OUT), jnp.float32)).astype(jnp.bfloat16)
    labels = jax.random.randint(sub_keys[3], (global_rows,), 0, CLASSES, jnp.int32)
    w_conv = C_MID ** -0.5 * jax.random.normal(sub_keys[4], (C_MID, C_OUT), jnp.float32)
    bn_gamma = jax.random.uniform(sub_keys[5], (C_OUT,), jnp.float32, 0.5, 1.5)
    bn_beta = 0.5 * jax.random.normal(sub_keys[6], (C_OUT,), jnp.float32)
    w_fc = C_OUT ** -0.5 * jax.random.normal(sub_keys[7], (C_OUT, CLASSES), jnp.float32)
    fc_bias = 0.5 * jax.random.normal(sub_keys[8], (CLASSES,), jnp.float32)
    vel_conv = 0.001 * step_scale * C_MID ** -0.5 * jax.random.normal(sub_keys[9], (C_MID, C_OUT), jnp.float32)
    vel_gamma = 0.5 * step_scale * (global_rows * C_OUT) ** -0.5 * jax.random.normal(sub_keys[10], (C_OUT,), jnp.float32)
    vel_beta = 0.5 * step_scale * (global_rows * C_OUT) ** -0.5 * jax.random.normal(sub_keys[11], (C_OUT,), jnp.float32)
    vel_fc = 0.001 * step_scale * C_OUT ** -0.5 * jax.random.normal(sub_keys[12], (C_OUT, CLASSES), jnp.float32)
    vel_bias = 0.9 * step_scale * (global_rows * CLASSES) ** -0.5 * jax.random.normal(sub_keys[13], (CLASSES,), jnp.float32)
    learn_rate = jax.random.uniform(sub_keys[14], (), jnp.float32, 1.0, 4.0)
    return {'act_in': act_in, 'shortcut': shortcut, 'labels': labels, 'w_conv': w_conv, 'bn_gamma': bn_gamma, 'bn_beta': bn_beta, 'w_fc': w_fc, 'fc_bias': fc_bias, 'vel_conv': vel_conv, 'vel_gamma': vel_gamma, 'vel_beta': vel_beta, 'vel_fc': vel_fc, 'vel_bias': vel_bias, 'learn_rate': learn_rate}


def group_loss(params, act_grp, short_grp, label_grp):
    w_conv, bn_gamma, bn_beta, w_fc, fc_bias = params
    pos_count = B_DEV * SIDE * SIDE
    conv_out = jnp.dot(act_grp.reshape(pos_count, C_MID), w_conv.astype(jnp.bfloat16), preferred_element_type=jnp.float32)
    batch_mean = jnp.mean(conv_out, axis=0)
    centered = conv_out - batch_mean
    batch_var = jnp.mean(jnp.square(centered), axis=0)
    x_hat = centered * lax.rsqrt(batch_var + BN_EPS)
    activ = jax.nn.relu(x_hat * bn_gamma + bn_beta + short_grp.reshape(pos_count, C_OUT).astype(jnp.float32))
    pooled = jnp.mean(activ.reshape(B_DEV, SIDE * SIDE, C_OUT), axis=1)
    logits = jnp.dot(pooled.astype(jnp.bfloat16), w_fc.astype(jnp.bfloat16), preferred_element_type=jnp.float32) + fc_bias
    log_prob = jax.nn.log_softmax(logits, axis=-1)
    one_hot_lab = (label_grp[:, None] == jnp.arange(CLASSES)[None, :]).astype(jnp.float32)
    target = SMOOTHING / CLASSES + (1.0 - SMOOTHING) * one_hot_lab
    return -jnp.sum(target * log_prob)


def lars_update(weight, gradient, velocity, learn_rate):
    w_norm = jnp.sqrt(jnp.sum(jnp.square(weight)))
    g_norm = jnp.sqrt(jnp.sum(jnp.square(gradient)))
    trust = TRUST_COEF * w_norm / (g_norm + WEIGHT_DECAY * w_norm)
    new_vel = MOMENTUM * velocity + learn_rate * trust * (gradient + WEIGHT_DECAY * weight)
    return weight - new_vel, new_vel


def reference(act_in, shortcut, labels, w_conv, bn_gamma, bn_beta, w_fc, fc_bias, vel_conv, vel_gamma, vel_beta, vel_fc, vel_bias, learn_rate):
    params = (w_conv, bn_gamma, bn_beta, w_fc, fc_bias)
    grad_fn = jax.value_and_grad(group_loss)
    global_rows = DP * B_DEV

    def scan_body(carry, group_batch):
        loss_sum, grad_sum = carry
        loss_val, grads = grad_fn(params, group_batch[0], group_batch[1], group_batch[2])
        return (loss_sum + loss_val, jax.tree.map(jnp.add, grad_sum, grads)), None

    init_carry = (jnp.zeros((), jnp.float32), jax.tree.map(jnp.zeros_like, params))
    group_data = (act_in.reshape(DP, B_DEV, SIDE, SIDE, C_MID), shortcut.reshape(DP, B_DEV, SIDE, SIDE, C_OUT), labels.reshape(DP, B_DEV))
    (loss_sum, grad_sum), unused_out = lax.scan(scan_body, init_carry, group_data)
    g_conv, g_gamma, g_beta, g_fc, g_bias = [grad_part / global_rows for grad_part in grad_sum]
    conv_new, conv_vel_new = lars_update(w_conv, g_conv, vel_conv, learn_rate)
    fc_new, fc_vel_new = lars_update(w_fc, g_fc, vel_fc, learn_rate)
    gamma_vel_new = MOMENTUM * vel_gamma + learn_rate * g_gamma
    beta_vel_new = MOMENTUM * vel_beta + learn_rate * g_beta
    bias_vel_new = MOMENTUM * vel_bias + learn_rate * g_bias
    return (conv_new, bn_gamma - gamma_vel_new, bn_beta - beta_vel_new, fc_new, fc_bias - bias_vel_new, conv_vel_new, gamma_vel_new, beta_vel_new, fc_vel_new, bias_vel_new, loss_sum / global_rows)
```

```python
import functools

import jax
import jax.numpy as jnp
from jax import lax
from jax.experimental import pallas as pl
from jax.experimental.pallas import tpu as pltpu
from jax.sharding import PartitionSpec as P

BN_EPS = 1e-5
SMOOTHING = 0.1
MOMENTUM = 0.9
TRUST_COEF = 0.001
WEIGHT_DECAY = 5e-5

F32 = jnp.float32
UR = 128
CS = 2
DEPTH = 3
ORDER = (3, 2, 1, 0, 7, 6, 5, 4)
MESH_ID = pl.DeviceIdType.MESH


def bytes_wait(ref, sem):
    pltpu.make_async_copy(ref, ref, sem).wait()


def reduce_kernel(n_dev, fc_rows, fc_units, n_units, gf_ref, gc_ref, of_ref, oc_ref, nrm_ref,
                  g, ba, bm, acc, ld, r0, r1, r2, r3, r4, r5, r6, r7, send, osem, credit):
    me = lax.axis_index('dp')
    core = me % 2
    zc = me // 8
    partner = me + 1 - 2 * core
    cols = g.shape[2]
    h, q, e = UR // 2, UR // 4, UR // 16
    mine = pl.ds(pl.multiple_of(core * UR, 8), UR)
    other = pl.ds(pl.multiple_of((1 - core) * UR, 8), UR)

    def rows(off, size):
        return pl.ds(pl.multiple_of(off, 8), size)

    def remote(src, dst, u, sem, dev):
        pltpu.make_async_remote_copy(src_ref=src, dst_ref=dst, send_sem=send.at[u], recv_sem=sem.at[u],
                                     device_id=(dev,), device_id_type=MESH_ID).start()

    def grant(k, u, dev):
        pl.semaphore_signal(credit.at[k, u], inc=1, device_id=(dev,), device_id_type=MESH_ID)

    class Place:
        def __init__(self, u):
            s_a = 2 + 2 * (u % 2)
            s_b = 6 - s_a
            bit_a = (me // s_a) % 2
            self.bit_b = (me // s_b) % 2
            self.dev_a = me + s_a * (1 - 2 * bit_a)
            self.dev_b = me + s_b * (1 - 2 * self.bit_b)
            self.keep_a = core * UR + bit_a * h
            self.give_a = core * UR + (1 - bit_a) * h
            self.quarter = self.keep_a + self.bit_b * q

    def z_peers():
        return [(d, (zc + d) % 4, (me + 8 * d) % n_dev) for d in (1, 3, 2)]

    barrier = pltpu.get_barrier_semaphore()

    def hello(d, c):
        pl.semaphore_signal(barrier, inc=1, device_id=((me + d) % n_dev,), device_id_type=MESH_ID)
        return c
    lax.fori_loop(1, n_dev, hello, 0)

    def hbm_slice(u, half):
        return rows((u // CS) * 2 * UR + half * UR, UR), pl.ds(pl.multiple_of((u % CS) * cols, 128), cols)

    def load_from(ref, first, last):
        def step(u, c):
            i, j = hbm_slice(u - first, core)
            pltpu.make_async_copy(ref.at[i, j], g.at[u, mine], ld.at[u]).start()
            return c
        lax.fori_loop(first, last, step, 0)

    def pair_from(ref, first, last):
        def step(u, c):
            i, j = hbm_slice(u - first, 1 - core)
            remote(ref.at[i, j], g.at[u, mine], u, r0, partner)
            return c
        lax.fori_loop(first, last, step, 0)

    load_from(gf_ref, 0, fc_units)
    load_from(gc_ref, fc_units, n_units)
    acc[...] = jnp.zeros_like(acc)
    pl.semaphore_wait(barrier, n_dev - 1)
    pair_from(gf_ref, 0, fc_units)
    pair_from(gc_ref, fc_units, n_units)

    def stage0(u):
        p = Place(u)
        bytes_wait(g.at[u, mine], ld.at[u])
        bytes_wait(g.at[u, mine], send.at[u])
        bytes_wait(g.at[u, other], r0.at[u])
        g[u, mine] += g[u, other]
        grant(0, u, partner)
        remote(g.at[u, rows(p.give_a, h)], ba.at[u], u, r1, p.dev_a)

    def stage1(u):
        p = Place(u)
        bytes_wait(ba.at[u], send.at[u])
        grant(1, u, p.dev_a)
        bytes_wait(ba.at[u], r1.at[u])
        g[u, rows(p.keep_a, h)] += ba[u]
        remote(g.at[u, rows(p.keep_a + (1 - p.bit_b) * q, q)], bm.at[u, pl.ds(0, q)], u, r2, p.dev_b)

    def stage2(u):
        p = Place(u)
        bytes_wait(bm.at[u, pl.ds(0, q)], send.at[u])
        grant(2, u, p.dev_b)
        bytes_wait(bm.at[u, pl.ds(0, q)], r2.at[u])
        g[u, rows(p.quarter, q)] += bm[u, pl.ds(0, q)]
        for d, to, dev in z_peers():
            remote(g.at[u, rows(p.quarter + to * e, e)], bm.at[u, pl.ds(q + (d - 1) * e, e)], u, r3, dev)

    def stage3(u):
        p = Place(u)
        bytes_wait(bm.at[u, pl.ds(q, 3 * e)], send.at[u])
        for _, _, dev in z_peers():
            grant(3, u, dev)
        bytes_wait(bm.at[u, pl.ds(q, 3 * e)], r3.at[u])
        left = rows(p.quarter + zc * e, e)
        g[u, left] = (g[u, left] + bm[u, pl.ds(q, e)]) + (bm[u, pl.ds(q + e, e)] + bm[u, pl.ds(q + 2 * e, e)])
        pl.semaphore_wait(credit.at[3, u], 3)
        for _, _, dev in z_peers():
            remote(g.at[u, left], g.at[u, left], u, r4, dev)

    def stage4(u):
        p = Place(u)
        bytes_wait(bm.at[u, pl.ds(q, 3 * e)], send.at[u])
        bytes_wait(bm.at[u, pl.ds(q, 3 * e)], r4.at[u])
        pl.semaphore_wait(credit.at[2, u], 1)
        block = rows(p.quarter, q)
        remote(g.at[u, block], g.at[u, block], u, r5, p.dev_b)

    def stage5(u):
        p = Place(u)
        bytes_wait(bm.at[u, pl.ds(0, q)], send.at[u])
        bytes_wait(bm.at[u, pl.ds(0, q)], r5.at[u])
        pl.semaphore_wait(credit.at[1, u], 1)
        block = rows(p.keep_a, h)
        remote(g.at[u, block], g.at[u, block], u, r6, p.dev_a)

    def stage6(u):
        bytes_wait(ba.at[u], send.at[u])
        bytes_wait(ba.at[u], r6.at[u])
        pl.semaphore_wait(credit.at[0, u], 1)
        remote(g.at[u, mine], g.at[u, mine], u, r7, partner)

    def stage7(u):
        bytes_wait(g.at[u, mine], send.at[u])
        bytes_wait(g.at[u, other], r7.at[u])
        is_fc = u < fc_units

        def out(ref, v, k):
            i, j = hbm_slice(v, 0)
            pltpu.make_async_copy(g.at[u], ref.at[rows((v // CS) * 2 * UR, 2 * UR), j], osem.at[k]).start()
        pl.when(is_fc)(lambda: out(of_ref, u, 0))
        pl.when(jnp.logical_not(is_fc))(lambda: out(oc_ref, u - fc_units, 1))
        kind = jnp.where(is_fc, 0, 1)
        limit = jnp.where(is_fc, fc_rows - (u // CS) * 2 * UR, 2 * UR)

        def square(k, c):
            x = g[u, rows(k * 8, 8)]
            return c + jnp.where(k * 8 < limit, x * x, 0.0)
        acc[kind] += lax.fori_loop(0, 2 * UR // 8, square, jnp.zeros((8, cols), F32))

    stages = (stage0, stage1, stage2, stage3, stage4, stage5, stage6, stage7)

    def step(t, c):
        for s in ORDER:
            u = t - DEPTH * s
            pl.when(jnp.logical_and(u >= 0, u < n_units))(functools.partial(stages[s], u))
        return c
    lax.fori_loop(0, n_units + DEPTH * (len(stages) - 1), step, 0)

    nrm_ref[...] = acc[...]
    bytes_wait(of_ref, osem.at[0])
    bytes_wait(oc_ref, osem.at[1])


def reduce_all(grad_fc, grad_conv, fc_rows, n_dev):
    width = grad_conv.shape[1]
    cols = width // CS
    fc_units = grad_fc.shape[0] // (2 * UR) * CS
    n_units = fc_units + grad_conv.shape[0] // (2 * UR) * CS
    dma = pltpu.SemaphoreType.DMA
    hbm = pl.BlockSpec(memory_space=pl.ANY)
    return pl.pallas_call(
        functools.partial(reduce_kernel, n_dev, fc_rows, fc_units, n_units),
        out_shape=(jax.ShapeDtypeStruct(grad_fc.shape, F32), jax.ShapeDtypeStruct(grad_conv.shape, F32),
                   jax.ShapeDtypeStruct((2, 8, cols), F32)),
        in_specs=[hbm, hbm],
        out_specs=(hbm, hbm, pl.BlockSpec(memory_space=pltpu.VMEM)),
        scratch_shapes=[
            pltpu.VMEM((n_units, 2 * UR, cols), F32),
            pltpu.VMEM((n_units, UR // 2, cols), F32),
            pltpu.VMEM((n_units, UR * 7 // 16, cols), F32),
            pltpu.VMEM((2, 8, cols), F32),
        ] + [dma((n_units,))] * 10 + [dma((2,)), pltpu.SemaphoreType.REGULAR((4, n_units))],
        compiler_params=pltpu.CompilerParams(collective_id=0, has_side_effects=True, vmem_limit_bytes=48 * 2 ** 20),
        name='reduce_all',
    )(grad_fc, grad_conv)


def solution(mesh):
    groups = mesh.shape['dp']

    def local_step(act_in, shortcut, labels, w_conv, bn_gamma, bn_beta, w_fc, fc_bias, vel_conv, vel_gamma, vel_beta, vel_fc, vel_bias, learn_rate):
        per_dev, side, _, c_mid = act_in.shape
        c_out = shortcut.shape[3]
        classes = w_fc.shape[1]
        spatial = side * side
        pos_count = per_dev * spatial
        global_rows = per_dev * groups
        act_grid = act_in.transpose(1, 2, 0, 3).reshape(spatial, per_dev, c_mid)
        short_grid = shortcut.transpose(1, 2, 0, 3).reshape(spatial, per_dev, c_out)
        conv_out = jnp.einsum('pbc,cd->pbd', act_grid, w_conv.astype(jnp.bfloat16), preferred_element_type=F32)
        batch_mean = jnp.mean(conv_out, axis=(0, 1))
        centered = conv_out - batch_mean
        inv_std = lax.rsqrt(jnp.mean(jnp.square(centered), axis=(0, 1)) + BN_EPS)
        x_hat = centered * inv_std
        pre_act = x_hat * bn_gamma + bn_beta + short_grid.astype(F32)
        pooled = jnp.mean(jax.nn.relu(pre_act), axis=0)
        pooled_bf = pooled.astype(jnp.bfloat16)
        fc_bf = w_fc.astype(jnp.bfloat16)
        logits = jnp.dot(pooled_bf, fc_bf, preferred_element_type=F32) + fc_bias
        log_prob = jax.nn.log_softmax(logits, axis=-1)
        one_hot_lab = (labels[:, None] == jnp.arange(classes, dtype=jnp.int32)[None, :]).astype(F32)
        target = SMOOTHING / classes + (1.0 - SMOOTHING) * one_hot_lab
        loss_part = -jnp.sum(target * log_prob) / global_rows
        d_logits = (jnp.exp(log_prob) - target) / global_rows
        d_bias = jnp.sum(d_logits, axis=0)
        d_logits_bf = d_logits.astype(jnp.bfloat16)
        d_pool = jnp.einsum('bk,ck->bc', d_logits_bf, fc_bf, preferred_element_type=F32) / spatial
        d_pre = jnp.where(pre_act > 0, d_pool[None], 0.0)
        d_beta = jnp.sum(d_pre, axis=(0, 1))
        d_gamma = jnp.sum(d_pre * x_hat, axis=(0, 1))
        d_conv_out = (bn_gamma * inv_std) * (d_pre - d_beta / pos_count - x_hat * (d_gamma / pos_count))
        d_conv = jnp.einsum('pbc,pbd->cd', act_grid, d_conv_out.astype(jnp.bfloat16), preferred_element_type=F32)

        padded = -(-classes // (2 * UR)) * 2 * UR
        d_fc = jnp.einsum('bk,bc->kc', jnp.pad(d_logits_bf, ((0, 0), (0, padded - classes))), pooled_bf, preferred_element_type=F32)
        last = jnp.concatenate([d_bias, loss_part[None], jnp.zeros((c_out - classes - 1,), F32)])
        small = jnp.concatenate([d_gamma[None], d_beta[None], last[None], jnp.zeros((5, c_out), F32)])
        d_fc = lax.dynamic_update_slice(d_fc, small, (classes, 0))

        g_fc, g_conv, sq = reduce_all(d_fc, d_conv, classes, groups)
        small = g_fc[classes:classes + 3]
        g_gamma, g_beta, g_bias, loss_val = small[0], small[1], small[2, :classes], small[2, classes]
        sq = jnp.sum(sq, axis=(1, 2))

        def lars(weight, gradient, velocity, g_sq):
            w_norm = jnp.sqrt(jnp.sum(jnp.square(weight)))
            trust = TRUST_COEF * w_norm / (jnp.sqrt(g_sq) + WEIGHT_DECAY * w_norm)
            new_vel = MOMENTUM * velocity + learn_rate * trust * (gradient + WEIGHT_DECAY * weight)
            return weight - new_vel, new_vel

        conv_new, conv_vel_new = lars(w_conv, g_conv, vel_conv, sq[1])
        fc_new, fc_vel_new = lars(w_fc.T, g_fc[:classes], vel_fc.T, sq[0])
        gamma_vel_new = MOMENTUM * vel_gamma + learn_rate * g_gamma
        beta_vel_new = MOMENTUM * vel_beta + learn_rate * g_beta
        bias_vel_new = MOMENTUM * vel_bias + learn_rate * g_bias
        return (conv_new, bn_gamma - gamma_vel_new, bn_beta - beta_vel_new, fc_new.T, fc_bias - bias_vel_new, conv_vel_new, gamma_vel_new, beta_vel_new, fc_vel_new.T, bias_vel_new, loss_val)

    return jax.shard_map(local_step, mesh=mesh, in_specs=(P('dp'),) * 3 + (P(),) * 11, out_specs=(P(),) * 11, check_vma=False)
```

```python
import functools

import jax
import jax.numpy as jnp
from jax import lax
from jax.experimental import pallas as pl
from jax.experimental.pallas import tpu as pltpu
from jax.sharding import PartitionSpec as P

BN_EPS = 1e-5
SMOOTHING = 0.1
MOMENTUM = 0.9
TRUST_COEF = 0.001
WEIGHT_DECAY = 5e-5

F32 = jnp.float32
UR = 128
CS = 2
DEPTH = 3
SPOT_SLOTS = 4
DOT_COLS = 256
DB = 256
ORDER = (3, 2, 1, 0, 7, 6, 5, 4)
MESH_ID = pl.DeviceIdType.MESH


def bytes_wait(ref, sem):
    pltpu.make_async_copy(ref, ref, sem).wait()


def reduce_kernel(n_dev, fc_rows, fc_units, n_units, gf_ref, a_ref, xh_ref, s_ref, gp_ref, vec_ref, of_ref, oc_ref, nrm_ref,
                  g, ba, bm, acc, dz, abuf, stg, xbuf, sbuf,
                  ld, r0, r1, r2, r3, r4, r5, r6, r7, send, osem, asem, xsem, ssem, credit):
    me = lax.axis_index('dp')
    core = me % 2
    zc = me // 8
    partner = me + 1 - 2 * core
    cols = g.shape[2]
    h, q, e = UR // 2, UR // 4, UR // 16
    mine = pl.ds(pl.multiple_of(core * UR, 8), UR)
    other = pl.ds(pl.multiple_of((1 - core) * UR, 8), UR)

    def rows(off, size):
        return pl.ds(pl.multiple_of(off, 8), size)

    def remote(src, dst, u, sem, dev):
        pltpu.make_async_remote_copy(src_ref=src, dst_ref=dst, send_sem=send.at[u], recv_sem=sem.at[u],
                                     device_id=(dev,), device_id_type=MESH_ID).start()

    def grant(k, u, dev):
        pl.semaphore_signal(credit.at[k, u], inc=1, device_id=(dev,), device_id_type=MESH_ID)

    class Place:
        def __init__(self, u):
            s_a = 2 + 2 * (u % 2)
            s_b = 6 - s_a
            bit_a = (me // s_a) % 2
            self.bit_b = (me // s_b) % 2
            self.dev_a = me + s_a * (1 - 2 * bit_a)
            self.dev_b = me + s_b * (1 - 2 * self.bit_b)
            self.keep_a = core * UR + bit_a * h
            self.give_a = core * UR + (1 - bit_a) * h
            self.quarter = self.keep_a + self.bit_b * q

    def z_peers():
        return [(d, (zc + d) % 4, (me + 8 * d) % n_dev) for d in (1, 3, 2)]

    barrier = pltpu.get_barrier_semaphore()

    def hello(d, c):
        pl.semaphore_signal(barrier, inc=1, device_id=((me + d) % n_dev,), device_id_type=MESH_ID)
        return c
    lax.fori_loop(1, n_dev, hello, 0)

    def hbm_slice(u, half):
        return rows((u // CS) * 2 * UR + half * UR, UR), pl.ds(pl.multiple_of((u % CS) * cols, 128), cols)

    def load_from(ref, first, last):
        def step(u, c):
            i, j = hbm_slice(u - first, core)
            pltpu.make_async_copy(ref.at[i, j], g.at[u, mine], ld.at[u]).start()
            return c
        lax.fori_loop(first, last, step, 0)

    def pair_from(ref, first, last):
        def step(u, c):
            i, j = hbm_slice(u - first, 1 - core)
            remote(ref.at[i, j], g.at[u, mine], u, r0, partner)
            return c
        lax.fori_loop(first, last, step, 0)

    spots, images = xh_ref.shape[0], xh_ref.shape[1]
    pieces = fc_units - 1
    per_piece = spots // pieces
    assert per_piece * pieces == spots

    def fetch_spot(p):
        slot = p % SPOT_SLOTS
        pltpu.make_async_copy(xh_ref.at[p], xbuf.at[slot], xsem.at[slot]).start()
        pltpu.make_async_copy(s_ref.at[p], sbuf.at[slot], ssem.at[slot]).start()

    def fetch_a(k):
        for part, half in ((0, core), (1, 1 - core)):
            pltpu.make_async_copy(a_ref.at[:, pl.ds(pl.multiple_of(k * 2 * UR + half * UR, 128), UR)],
                                  abuf.at[k % 2, :, pl.ds(part * UR, UR)], asem.at[k % 2, part]).start()

    for p in range(SPOT_SLOTS):
        fetch_spot(p)
    load_from(gf_ref, 0, fc_units)
    fetch_a(0)
    fetch_a(1)
    acc[...] = jnp.zeros_like(acc)
    pl.semaphore_wait(barrier, n_dev - 1)
    pair_from(gf_ref, 0, fc_units)

    def spot_step(p, c):
        slot = p % SPOT_SLOTS
        bytes_wait(xbuf.at[slot], xsem.at[slot])
        bytes_wait(sbuf.at[slot], ssem.at[slot])

        def group(r, c):
            x = xbuf[slot, pl.ds(pl.multiple_of(r * 16, 16), 16)]
            pre = x * vec_ref[0:1] + vec_ref[1:2] + sbuf[slot, pl.ds(pl.multiple_of(r * 16, 16), 16)].astype(F32)
            d = jnp.where(pre > 0, gp_ref[pl.ds(pl.multiple_of(r * 16, 16), 16)], 0.0) - vec_ref[2:3] - x * vec_ref[3:4]
            dz[pl.ds(pl.multiple_of(p * images + r * 16, 16), 16)] = d.astype(jnp.bfloat16)
            return c
        lax.fori_loop(0, images // 16, group, 0)
        pl.when(p + SPOT_SLOTS < spots)(lambda: fetch_spot(p + SPOT_SLOTS))
        return c

    def weight_grad(u):
        v = u - fc_units
        k = v // CS
        cb = v % CS

        @pl.when(cb == 0)
        def _():
            for part in range(2):
                bytes_wait(abuf.at[k % 2, :, pl.ds(part * UR, UR)], asem.at[k % 2, part])

        def block(n, c):
            col = pl.multiple_of(n * DOT_COLS, 128)
            out = lax.dot_general(abuf[k % 2], dz[:, pl.ds(pl.multiple_of(cb * cols + col, 128), DOT_COLS)],
                                  (((0,), (0,)), ((), ())), preferred_element_type=F32)
            g[u, mine, pl.ds(col, DOT_COLS)] = out[:UR]
            stg[u % 4, :, pl.ds(col, DOT_COLS)] = out[UR:]
            return c
        lax.fori_loop(0, cols // DOT_COLS, block, 0)
        remote(stg.at[u % 4], g.at[u, mine], u, r0, partner)

        @pl.when(jnp.logical_and(cb == CS - 1, v + 1 + CS < n_units - fc_units))
        def _():
            fetch_a(k + 2)

    def stage0(u):
        p = Place(u)
        pl.when(u < fc_units)(lambda: bytes_wait(g.at[u, mine], ld.at[u]))
        bytes_wait(g.at[u, mine], send.at[u])
        bytes_wait(g.at[u, other], r0.at[u])
        g[u, mine] += g[u, other]
        grant(0, u, partner)
        remote(g.at[u, rows(p.give_a, h)], ba.at[u], u, r1, p.dev_a)

    def stage1(u):
        p = Place(u)
        bytes_wait(ba.at[u], send.at[u])
        grant(1, u, p.dev_a)
        bytes_wait(ba.at[u], r1.at[u])
        g[u, rows(p.keep_a, h)] += ba[u]
        remote(g.at[u, rows(p.keep_a + (1 - p.bit_b) * q, q)], bm.at[u, pl.ds(0, q)], u, r2, p.dev_b)

    def stage2(u):
        p = Place(u)
        bytes_wait(bm.at[u, pl.ds(0, q)], send.at[u])
        grant(2, u, p.dev_b)
        bytes_wait(bm.at[u, pl.ds(0, q)], r2.at[u])
        g[u, rows(p.quarter, q)] += bm[u, pl.ds(0, q)]
        for d, to, dev in z_peers():
            remote(g.at[u, rows(p.quarter + to * e, e)], bm.at[u, pl.ds(q + (d - 1) * e, e)], u, r3, dev)

    def stage3(u):
        p = Place(u)
        bytes_wait(bm.at[u, pl.ds(q, 3 * e)], send.at[u])
        for _, _, dev in z_peers():
            grant(3, u, dev)
        bytes_wait(bm.at[u, pl.ds(q, 3 * e)], r3.at[u])
        left = rows(p.quarter + zc * e, e)
        g[u, left] = (g[u, left] + bm[u, pl.ds(q, e)]) + (bm[u, pl.ds(q + e, e)] + bm[u, pl.ds(q + 2 * e, e)])
        pl.semaphore_wait(credit.at[3, u], 3)
        for _, _, dev in z_peers():
            remote(g.at[u, left], g.at[u, left], u, r4, dev)

    def stage4(u):
        p = Place(u)
        bytes_wait(bm.at[u, pl.ds(q, 3 * e)], send.at[u])
        bytes_wait(bm.at[u, pl.ds(q, 3 * e)], r4.at[u])
        pl.semaphore_wait(credit.at[2, u], 1)
        block = rows(p.quarter, q)
        remote(g.at[u, block], g.at[u, block], u, r5, p.dev_b)

    def stage5(u):
        p = Place(u)
        bytes_wait(bm.at[u, pl.ds(0, q)], send.at[u])
        bytes_wait(bm.at[u, pl.ds(0, q)], r5.at[u])
        pl.semaphore_wait(credit.at[1, u], 1)
        block = rows(p.keep_a, h)
        remote(g.at[u, block], g.at[u, block], u, r6, p.dev_a)

    def stage6(u):
        bytes_wait(ba.at[u], send.at[u])
        bytes_wait(ba.at[u], r6.at[u])
        pl.semaphore_wait(credit.at[0, u], 1)
        remote(g.at[u, mine], g.at[u, mine], u, r7, partner)

    def stage7(u):
        bytes_wait(g.at[u, mine], send.at[u])
        bytes_wait(g.at[u, other], r7.at[u])
        is_fc = u < fc_units

        def out(ref, v, k):
            i, j = hbm_slice(v, 0)
            pltpu.make_async_copy(g.at[u], ref.at[rows((v // CS) * 2 * UR, 2 * UR), j], osem.at[k]).start()
        pl.when(is_fc)(lambda: out(of_ref, u, 0))
        pl.when(jnp.logical_not(is_fc))(lambda: out(oc_ref, u - fc_units, 1))
        kind = jnp.where(is_fc, 0, 1)
        limit = jnp.where(is_fc, fc_rows - (u // CS) * 2 * UR, 2 * UR)

        def square(k, c):
            x = g[u, rows(k * 8, 8)]
            return c + jnp.where(k * 8 < limit, x * x, 0.0)
        acc[kind] += lax.fori_loop(0, 2 * UR // 8, square, jnp.zeros((8, cols), F32))

    stages = (stage0, stage1, stage2, stage3, stage4, stage5, stage6, stage7)

    def step(t, c):
        for s in ORDER:
            u = t - DEPTH * s
            pl.when(jnp.logical_and(u >= 0, u < n_units))(functools.partial(stages[s], u))

        @pl.when(t < pieces)
        def _():
            lax.fori_loop(t * per_piece, (t + 1) * per_piece, spot_step, 0)
        pl.when(jnp.logical_and(t >= pieces, t + 1 < n_units))(lambda: weight_grad(t + 1))
        return c
    lax.fori_loop(0, n_units + DEPTH * (len(stages) - 1), step, 0)

    nrm_ref[...] = acc[...]
    bytes_wait(of_ref, osem.at[0])
    bytes_wait(oc_ref, osem.at[1])


def reduce_all(grad_fc, act, x_hat, short, gate, vec, fc_rows, n_dev):
    rows_a, c_mid = act.shape
    width = x_hat.shape[2]
    cols = width // CS
    fc_units = grad_fc.shape[0] // (2 * UR) * CS
    n_units = fc_units + c_mid // (2 * UR) * CS
    dma = pltpu.SemaphoreType.DMA
    hbm = pl.BlockSpec(memory_space=pl.ANY)
    vmem = pl.BlockSpec(memory_space=pltpu.VMEM)
    bf16 = jnp.bfloat16
    images = x_hat.shape[1]
    return pl.pallas_call(
        functools.partial(reduce_kernel, n_dev, fc_rows, fc_units, n_units),
        out_shape=(jax.ShapeDtypeStruct(grad_fc.shape, F32), jax.ShapeDtypeStruct((c_mid, width), F32),
                   jax.ShapeDtypeStruct((2, 8, cols), F32)),
        in_specs=[hbm, hbm, hbm, hbm, vmem, vmem],
        out_specs=(hbm, hbm, vmem),
        scratch_shapes=[
            pltpu.VMEM((n_units, 2 * UR, cols), F32),
            pltpu.VMEM((n_units, UR // 2, cols), F32),
            pltpu.VMEM((n_units, UR * 7 // 16, cols), F32),
            pltpu.VMEM((2, 8, cols), F32),
            pltpu.VMEM((rows_a, width), bf16),
            pltpu.VMEM((2, rows_a, 2 * UR), bf16),
            pltpu.VMEM((4, UR, cols), F32),
            pltpu.VMEM((SPOT_SLOTS, images, width), F32),
            pltpu.VMEM((SPOT_SLOTS, images, width), bf16),
        ] + [dma((n_units,))] * 10 + [dma((2,)), dma((2, 2)), dma((SPOT_SLOTS,)), dma((SPOT_SLOTS,)), pltpu.SemaphoreType.REGULAR((4, n_units))],
        compiler_params=pltpu.CompilerParams(collective_id=0, has_side_effects=True, vmem_limit_bytes=67043328),
        name='reduce_all',
    )(grad_fc, act, x_hat, short, gate, vec)


def forward_kernel(blocks, global_rows, a_ref, w_ref, s_ref, gb_ref, lab_ref, bias_ref, wfc_ref, xh_ref, dfc_ref, gate_ref, vec_ref, wsq_ref, fsq_ref,
                   z0, z1, wb, stat, pool_s, cnt_s, sx_s, inv_s, big, fcb, sem):
    j = pl.program_id(0)
    spots, images, width = xh_ref.shape
    total = spots * images
    classes = wfc_ref.shape[0]
    load_fc = pltpu.make_async_copy(wfc_ref, big.at[pl.ds(0, classes)], sem.at[0])

    def run(now):
        w = w_ref[...]
        wb[...] = w.astype(jnp.bfloat16)
        wsq_ref[...] = jnp.sum((w * w).reshape(w.shape[0] // 8, 8, width), axis=0)
        out = jnp.dot(a_ref[...], wb[...], preferred_element_type=F32)
        now[...] = out.reshape(spots, images, width)
        mean = jnp.sum(out, axis=0, keepdims=True) / total
        d = out - mean
        var = jnp.sum(jnp.sum((d * d).reshape(total // 8, 8, width), axis=0), axis=0, keepdims=True) / total
        stat[0:1] = mean
        stat[1:2] = lax.rsqrt(var + BN_EPS)

    def finish(z):
        at = pl.ds(pl.multiple_of((j - 1) * width, 128), width)
        mean, inv = mean_inv
        gamma, beta = gb_ref[0:1, at], gb_ref[1:2, at]
        inv_s[0:1, at] = inv
        zero = jnp.zeros((8, width), F32)
        for r in range(0, images, 8):
            img = pl.ds(r, 8)
            pool, cnt, sx = zero, zero, zero
            for p in range(spots):
                x = (z[p, img] - mean) * inv
                xh_ref[p, img] = x
                pre = x * gamma + beta + s_ref[p, img].astype(F32)
                on = pre > 0
                pool += jnp.where(on, pre, 0.0)
                cnt += jnp.where(on, 1.0, 0.0)
                sx += jnp.where(on, x, 0.0)
            pool_s[img, at], cnt_s[img, at], sx_s[img, at] = pool, cnt, sx

    mean_inv = stat[0:1], stat[1:2]
    pl.when(j == 0)(load_fc.start)

    @pl.when(j == 0)
    def _():
        run(z0)

    @pl.when(jnp.logical_and(jnp.logical_and(j > 0, j < blocks), j % 2 == 0))
    def _():
        run(z0)
        finish(z1)

    @pl.when(jnp.logical_and(j < blocks, j % 2 == 1))
    def _():
        run(z1)
        finish(z0)

    @pl.when(j == blocks)
    def _():
        finish(z1 if blocks % 2 == 0 else z0)
        load_fc.wait()
        spread = gb_ref.shape[1]

        def pack(i, c):
            at = pl.ds(pl.multiple_of(i * 8, 8), 8)
            w = big[at]
            fcb[at] = w.astype(jnp.bfloat16)
            return c + w * w
        fsq_ref[...] = lax.fori_loop(0, classes // 8, pack, jnp.zeros((8, spread), F32))
        pooled = (pool_s[...] / spots).astype(jnp.bfloat16)
        wide = fcb[...]
        logits = lax.dot_general(pooled, wide, (((1,), (1,)), ((), ())), preferred_element_type=F32) + bias_ref[...]
        shifted = logits - jnp.max(logits, axis=1, keepdims=True)
        log_prob = shifted - jnp.log(jnp.sum(jnp.exp(shifted), axis=1, keepdims=True))
        hit = lab_ref[...] == lax.broadcasted_iota(jnp.int32, logits.shape, 1)
        target = SMOOTHING / classes + (1.0 - SMOOTHING) * jnp.where(hit, 1.0, 0.0)
        loss = -jnp.sum(target * log_prob) / global_rows
        d_logits = (jnp.exp(log_prob) - target) / global_rows
        d_bias = jnp.sum(d_logits, axis=0, keepdims=True)
        d_bf = d_logits.astype(jnp.bfloat16)
        big[pl.ds(0, classes)] = lax.dot_general(d_bf, pooled, (((0,), (0,)), ((), ())), preferred_element_type=F32)
        d_pool = lax.dot_general(d_bf, wide, (((1,), (0,)), ((), ())), preferred_element_type=F32) / spots
        d_beta = jnp.sum(d_pool * cnt_s[...], axis=0, keepdims=True)
        d_gamma = jnp.sum(d_pool * sx_s[...], axis=0, keepdims=True)
        gi = gb_ref[0:1] * inv_s[0:1]
        gate_ref[...] = d_pool * gi
        vec_ref[0:2] = gb_ref[0:2]
        vec_ref[2:3] = gi * (d_beta / total)
        vec_ref[3:4] = gi * (d_gamma / total)
        rest = big.shape[0] - classes
        big[pl.ds(classes, rest)] = jnp.zeros((rest, spread), F32)
        big[pl.ds(classes, 1)] = d_gamma
        big[pl.ds(classes + 1, 1)] = d_beta
        big[pl.ds(classes + 2, 1), pl.ds(0, classes)] = d_bias
        big[pl.ds(classes + 3, 1)] = jnp.full((1, spread), loss, F32)
        store = pltpu.make_async_copy(big, dfc_ref, sem.at[1])
        store.start()
        store.wait()


def forward(act, weight, short, scale, labels, bias, w_fct, global_rows):
    rows_a, c_mid = act.shape
    spots, images, c_out = short.shape
    classes = w_fct.shape[0]
    padded = -(-classes // (2 * UR)) * 2 * UR
    blocks = c_out // DB
    def now(j):
        return 0, jnp.minimum(j, blocks - 1)
    def late3(j):
        return 0, 0, jnp.maximum(j - 1, 0)
    def whole(shape):
        return pl.BlockSpec(shape, lambda j: (0,) * len(shape), pipeline_mode=pl.Buffered(1))
    hbm = pl.BlockSpec(memory_space=pl.ANY)
    rows8 = jax.ShapeDtypeStruct((8, c_out), F32)
    plane = pltpu.VMEM((images, c_out), F32)
    return pl.pallas_call(
        functools.partial(forward_kernel, blocks, global_rows),
        grid=(blocks + 1,),
        out_shape=(jax.ShapeDtypeStruct((spots, images, c_out), F32), jax.ShapeDtypeStruct((padded, c_out), F32),
                   jax.ShapeDtypeStruct((images, c_out), F32), rows8, rows8, rows8),
        in_specs=[whole((rows_a, c_mid)), pl.BlockSpec((c_mid, DB), now), pl.BlockSpec((spots, images, DB), late3),
                  whole((8, c_out)), whole(labels.shape), whole(bias.shape), hbm],
        out_specs=(pl.BlockSpec((spots, images, DB), late3), hbm, pl.BlockSpec((images, c_out), lambda j: (0, 0)),
                   pl.BlockSpec((8, c_out), lambda j: (0, 0)), pl.BlockSpec((8, DB), now), pl.BlockSpec((8, c_out), lambda j: (0, 0))),
        scratch_shapes=[pltpu.VMEM((spots, images, DB), F32)] * 2 + [pltpu.VMEM((c_mid, DB), jnp.bfloat16), pltpu.VMEM((8, DB), F32),
                        plane, plane, plane, pltpu.VMEM((8, c_out), F32), pltpu.VMEM((padded, c_out), F32),
                        pltpu.VMEM((classes, c_out), jnp.bfloat16), pltpu.SemaphoreType.DMA((2,))],
        compiler_params=pltpu.CompilerParams(vmem_limit_bytes=63 * 2 ** 20),
        name='forward',
    )(act, weight, short, scale, labels, bias, w_fct)


def update_kernel(conv_steps, lr_ref, nrm_ref, csq_ref, fsq_ref, gc_ref, wc_ref, vc_ref, gf_ref, wf_ref, vf_ref,
                  wc_new, vc_new, wf_new, vf_new, rate):
    i = pl.program_id(0)
    lr = lr_ref[0, 0]

    @pl.when(i == 0)
    def _():
        for k, sq_ref in ((0, csq_ref), (1, fsq_ref)):
            w_norm = jnp.sqrt(jnp.sum(jnp.sum(sq_ref[...], axis=0, keepdims=True), axis=1, keepdims=True))
            g_norm = jnp.sqrt(jnp.sum(jnp.sum(nrm_ref[1 - k], axis=0, keepdims=True), axis=1, keepdims=True))
            rate[k:k + 1] = jnp.broadcast_to(lr * (TRUST_COEF * w_norm / (g_norm + WEIGHT_DECAY * w_norm)), (1, 128))

    def apply(k, g_ref, w_ref, v_ref, w_out, v_out):
        scale = rate[k:k + 1, 0:1]

        def some(r, c):
            at = pl.ds(pl.multiple_of(r * 8, 8), 8)
            w = w_ref[at]
            v = MOMENTUM * v_ref[at] + scale * (g_ref[at] + WEIGHT_DECAY * w)
            v_out[at] = v
            w_out[at] = w - v
            return c
        lax.fori_loop(0, w_ref.shape[0] // 8, some, 0, unroll=True)

    pl.when(i < conv_steps)(lambda: apply(0, gc_ref, wc_ref, vc_ref, wc_new, vc_new))
    pl.when(i >= conv_steps)(lambda: apply(1, gf_ref, wf_ref, vf_ref, wf_new, vf_new))


def update(rate, norms, conv_sq, fc_sq, g_conv, w_conv, v_conv, g_fc, w_fct, v_fct):
    width = w_conv.shape[1]
    conv_rows, fc_rows = 256, 200
    conv_steps, fc_steps = w_conv.shape[0] // conv_rows, w_fct.shape[0] // fc_rows
    conv = pl.BlockSpec((conv_rows, width), lambda i: (jnp.minimum(i, conv_steps - 1), 0))
    fc = pl.BlockSpec((fc_rows, width), lambda i: (jnp.maximum(i - conv_steps, 0), 0))
    vmem = pl.BlockSpec(memory_space=pltpu.VMEM)
    return pl.pallas_call(
        functools.partial(update_kernel, conv_steps),
        grid=(conv_steps + fc_steps,),
        out_shape=(jax.ShapeDtypeStruct(w_conv.shape, F32),) * 2 + (jax.ShapeDtypeStruct(w_fct.shape, F32),) * 2,
        in_specs=[pl.BlockSpec(memory_space=pltpu.SMEM), vmem, vmem, vmem, conv, conv, conv, fc, fc, fc],
        out_specs=(conv, conv, fc, fc),
        scratch_shapes=[pltpu.VMEM((8, 128), F32)],
        compiler_params=pltpu.CompilerParams(vmem_limit_bytes=60 * 2 ** 20),
        name='update',
    )(rate, norms, conv_sq, fc_sq, g_conv, w_conv, v_conv, g_fc, w_fct, v_fct)


def solution(mesh):
    groups = mesh.shape['dp']

    def local_step(act_in, shortcut, labels, w_conv, bn_gamma, bn_beta, w_fc, fc_bias, vel_conv, vel_gamma, vel_beta, vel_fc, vel_bias, learn_rate):
        per_dev, side, _, c_mid = act_in.shape
        c_out = shortcut.shape[3]
        classes = w_fc.shape[1]
        spatial = side * side
        pos_count = per_dev * spatial
        global_rows = per_dev * groups
        act = act_in.transpose(1, 2, 0, 3).reshape(pos_count, c_mid)
        short = shortcut.transpose(1, 2, 0, 3).reshape(spatial, per_dev, c_out)
        scale = jnp.concatenate([bn_gamma[None], bn_beta[None], jnp.zeros((6, c_out), F32)])
        x_hat, d_fc, gate, vec, conv_sq, fc_sq = forward(act, w_conv, short, scale, labels[:, None], fc_bias[None], w_fc.T, global_rows)
        g_fc, g_conv, norms = reduce_all(d_fc, act, x_hat, short, gate, vec, classes, groups)
        small = g_fc[classes:classes + 4]
        g_gamma, g_beta, g_bias, loss_val = small[0], small[1], small[2, :classes], small[3, 0]
        conv_new, conv_vel_new, fc_new, fc_vel_new = update(learn_rate[None, None], norms, conv_sq, fc_sq, g_conv, w_conv, vel_conv,
                                                            g_fc, w_fc.T, vel_fc.T)
        gamma_vel_new = MOMENTUM * vel_gamma + learn_rate * g_gamma
        beta_vel_new = MOMENTUM * vel_beta + learn_rate * g_beta
        bias_vel_new = MOMENTUM * vel_bias + learn_rate * g_bias
        return (conv_new, bn_gamma - gamma_vel_new, bn_beta - beta_vel_new, fc_new.T, fc_bias - bias_vel_new, conv_vel_new, gamma_vel_new, beta_vel_new, fc_vel_new.T, bias_vel_new, loss_val)

    return jax.shard_map(local_step, mesh=mesh, in_specs=(P('dp'),) * 3 + (P(),) * 11, out_specs=(P(),) * 11, check_vma=False)
```

```python
import functools

import jax
import jax.numpy as jnp
from jax import lax
from jax.experimental import pallas as pl
from jax.experimental.pallas import tpu as pltpu
from jax.sharding import PartitionSpec as P

BN_EPS = 1e-5
SMOOTHING = 0.1
MOMENTUM = 0.9
TRUST_COEF = 0.001
WEIGHT_DECAY = 5e-5

F32 = jnp.float32
UR = 128
CS = 2
OFFSETS = (0, 3, 5, 7, 9, 11, 13, 15, 18, 21)
SPOT_SLOTS = 4
DOT_COLS = 1024
DB = 256
PIECES = 7
LEVELS = 4
MESH_ID = pl.DeviceIdType.MESH


def bytes_wait(ref, sem):
    pltpu.make_async_copy(ref, ref, sem).wait()


def reduce_kernel(n_dev, fc_rows, fc_units, n_units, gf_ref, a_ref, xh_ref, s_ref, gp_ref, vec_ref, of_ref, oc_ref, nrm_ref,
                  g, ba, bm, acc, dz, abuf, stg, xbuf, sbuf,
                  ld, recv, send, osem, asem, xsem, ssem, credit):
    me = lax.axis_index('dp')
    core = me % 2
    partner = me + 1 - 2 * core
    cols = g.shape[2]
    size = [UR >> i for i in range(LEVELS + 1)]
    mine = pl.ds(pl.multiple_of(core * UR, 8), UR)
    other = pl.ds(pl.multiple_of((1 - core) * UR, 8), UR)

    def rows(off, size):
        return pl.ds(pl.multiple_of(off, 8), size)

    def remote(src, dst, u, k, dev):
        pltpu.make_async_remote_copy(src_ref=src, dst_ref=dst, send_sem=send.at[u], recv_sem=recv.at[k, u],
                                     device_id=(dev,), device_id_type=MESH_ID).start()

    def grant(k, u, dev):
        pl.semaphore_signal(credit.at[k, u], inc=1, device_id=(dev,), device_id_type=MESH_ID)

    def levels(u):
        s_a = 2 + 2 * (u % 2)
        keep = core * UR
        out = [(partner, keep, None)]
        for i, stride in enumerate((s_a, 8, 6 - s_a, 16), 1):
            bit = (me // stride) % 2
            give = keep + (1 - bit) * size[i]
            keep = keep + bit * size[i]
            out.append((me + stride * (1 - 2 * bit), keep, give))
        return out

    def landing(u, i):
        if i == 1:
            return ba.at[u]
        return bm.at[u, pl.ds(size[1] - size[i - 1], size[i])]

    barrier = pltpu.get_barrier_semaphore()

    def hello(d, c):
        pl.semaphore_signal(barrier, inc=1, device_id=((me + d) % n_dev,), device_id_type=MESH_ID)
        return c
    lax.fori_loop(1, n_dev, hello, 0)

    def hbm_slice(u, half):
        return rows((u // CS) * 2 * UR + half * UR, UR), pl.ds(pl.multiple_of((u % CS) * cols, 128), cols)

    def load_from(ref, first, last):
        def step(u, c):
            i, j = hbm_slice(u - first, core)
            pltpu.make_async_copy(ref.at[i, j], g.at[u, mine], ld.at[u]).start()
            return c
        lax.fori_loop(first, last, step, 0)

    def pair_from(ref, first, last):
        def step(u, c):
            i, j = hbm_slice(u - first, 1 - core)
            remote(ref.at[i, j], g.at[u, mine], u, 0, partner)
            return c
        lax.fori_loop(first, last, step, 0)

    spots, images = xh_ref.shape[0], xh_ref.shape[1]
    pieces = PIECES
    per_piece = spots // pieces
    assert per_piece * pieces == spots

    def fetch_spot(p):
        slot = p % SPOT_SLOTS
        pltpu.make_async_copy(xh_ref.at[p], xbuf.at[slot], xsem.at[slot]).start()
        pltpu.make_async_copy(s_ref.at[p], sbuf.at[slot], ssem.at[slot]).start()

    def fetch_a(k):
        for part, half in ((0, core), (1, 1 - core)):
            pltpu.make_async_copy(a_ref.at[:, pl.ds(pl.multiple_of(k * 2 * UR + half * UR, 128), UR)],
                                  abuf.at[k % 2, :, pl.ds(part * UR, UR)], asem.at[k % 2, part]).start()

    for p in range(SPOT_SLOTS):
        fetch_spot(p)
    load_from(gf_ref, 0, fc_units)
    fetch_a(0)
    fetch_a(1)
    acc[...] = jnp.zeros_like(acc)
    pl.semaphore_wait(barrier, n_dev - 1)
    pair_from(gf_ref, 0, fc_units)

    def spot_step(p, c):
        slot = p % SPOT_SLOTS
        bytes_wait(xbuf.at[slot], xsem.at[slot])
        bytes_wait(sbuf.at[slot], ssem.at[slot])

        def group(r, c):
            x = xbuf[slot, pl.ds(pl.multiple_of(r * 16, 16), 16)]
            pre = x * vec_ref[0:1] + vec_ref[1:2] + sbuf[slot, pl.ds(pl.multiple_of(r * 16, 16), 16)].astype(F32)
            d = jnp.where(pre > 0, gp_ref[pl.ds(pl.multiple_of(r * 16, 16), 16)], 0.0) - vec_ref[2:3] - x * vec_ref[3:4]
            dz[pl.ds(pl.multiple_of(p * images + r * 16, 16), 16)] = d.astype(jnp.bfloat16)
            return c
        lax.fori_loop(0, images // 16, group, 0)
        pl.when(p + SPOT_SLOTS < spots)(lambda: fetch_spot(p + SPOT_SLOTS))
        return c

    def weight_grad(u):
        v = u - fc_units
        k = v // CS
        cb = v % CS

        @pl.when(cb == 0)
        def _():
            for part in range(2):
                bytes_wait(abuf.at[k % 2, :, pl.ds(part * UR, UR)], asem.at[k % 2, part])

        def block(n, c):
            col = pl.multiple_of(n * DOT_COLS, 128)
            out = lax.dot_general(abuf[k % 2], dz[:, pl.ds(pl.multiple_of(cb * cols + col, 128), DOT_COLS)],
                                  (((0,), (0,)), ((), ())), preferred_element_type=F32)
            g[u, mine, pl.ds(col, DOT_COLS)] = out[:UR]
            stg[u % 4, :, pl.ds(col, DOT_COLS)] = out[UR:]
            return c
        lax.fori_loop(0, cols // DOT_COLS, block, 0)
        remote(stg.at[u % 4], g.at[u, mine], u, 0, partner)

        @pl.when(jnp.logical_and(cb == CS - 1, v + 1 + CS < n_units - fc_units))
        def _():
            fetch_a(k + 2)

    def reduce_stage(i, u):
        at = levels(u)
        dev, keep, _ = at[i]
        if i == 0:
            pl.when(u < fc_units)(lambda: bytes_wait(g.at[u, mine], ld.at[u]))
            bytes_wait(g.at[u, mine], send.at[u])
            bytes_wait(g.at[u, other], recv.at[0, u])
            g[u, mine] += g[u, other]
            grant(0, u, partner)
        else:
            bytes_wait(landing(u, i), send.at[u])
            grant(i, u, dev)
            bytes_wait(landing(u, i), recv.at[i, u])
            g[u, rows(keep, size[i])] += landing(u, i)[...]
        if i < LEVELS:
            dev, _, give = at[i + 1]
            remote(g.at[u, rows(give, size[i + 1])], landing(u, i + 1), u, i + 1, dev)
        else:
            gather_send(i, u, at)

    def gather_send(i, u, at):
        dev, keep, _ = at[i]
        pl.semaphore_wait(credit.at[i, u], 1)
        block = g.at[u, rows(keep, size[i])]
        remote(block, block, u, 2 * LEVELS + 1 - i, dev)

    def gather_stage(i, u):
        bytes_wait(landing(u, i), send.at[u])
        bytes_wait(landing(u, i), recv.at[2 * LEVELS + 1 - i, u])
        gather_send(i - 1, u, levels(u))

    def last_stage(u):
        bytes_wait(g.at[u, mine], send.at[u])
        bytes_wait(g.at[u, other], recv.at[2 * LEVELS + 1, u])
        is_fc = u < fc_units

        def out(ref, v, k):
            i, j = hbm_slice(v, 0)
            pltpu.make_async_copy(g.at[u], ref.at[rows((v // CS) * 2 * UR, 2 * UR), j], osem.at[k]).start()
        pl.when(is_fc)(lambda: out(of_ref, u, 0))
        pl.when(jnp.logical_not(is_fc))(lambda: out(oc_ref, u - fc_units, 1))
        kind = jnp.where(is_fc, 0, 1)
        limit = jnp.where(is_fc, fc_rows - (u // CS) * 2 * UR, 2 * UR)

        def square(k, c):
            x = g[u, rows(k * 8, 8)]
            return c + jnp.where(k * 8 < limit, x * x, 0.0)
        acc[kind] += lax.fori_loop(0, 2 * UR // 8, square, jnp.zeros((8, cols), F32))

    stages = ([functools.partial(reduce_stage, i) for i in range(LEVELS + 1)]
              + [functools.partial(gather_stage, i) for i in range(LEVELS, 0, -1)] + [last_stage])

    def step(t, c):
        for s in [*range(LEVELS, -1, -1), *range(2 * LEVELS + 1, LEVELS, -1)]:
            u = t - OFFSETS[s]
            pl.when(jnp.logical_and(u >= 0, u < n_units))(functools.partial(stages[s], u))

        @pl.when(t < pieces)
        def _():
            lax.fori_loop(t * per_piece, (t + 1) * per_piece, spot_step, 0)
        pl.when(jnp.logical_and(t + 1 >= fc_units, t + 1 < n_units))(lambda: weight_grad(t + 1))
        return c
    lax.fori_loop(0, n_units + OFFSETS[-1], step, 0)

    nrm_ref[...] = acc[...]
    bytes_wait(of_ref, osem.at[0])
    bytes_wait(oc_ref, osem.at[1])


def reduce_all(grad_fc, act, x_hat, short, gate, vec, fc_rows, n_dev):
    rows_a, c_mid = act.shape
    width = x_hat.shape[2]
    cols = width // CS
    fc_units = grad_fc.shape[0] // (2 * UR) * CS
    n_units = fc_units + c_mid // (2 * UR) * CS
    dma = pltpu.SemaphoreType.DMA
    hbm = pl.BlockSpec(memory_space=pl.ANY)
    vmem = pl.BlockSpec(memory_space=pltpu.VMEM)
    bf16 = jnp.bfloat16
    images = x_hat.shape[1]
    return pl.pallas_call(
        functools.partial(reduce_kernel, n_dev, fc_rows, fc_units, n_units),
        out_shape=(jax.ShapeDtypeStruct(grad_fc.shape, F32), jax.ShapeDtypeStruct((c_mid, width), F32),
                   jax.ShapeDtypeStruct((2, 8, cols), F32)),
        in_specs=[hbm, hbm, hbm, hbm, vmem, vmem],
        out_specs=(hbm, hbm, vmem),
        scratch_shapes=[
            pltpu.VMEM((n_units, 2 * UR, cols), F32),
            pltpu.VMEM((n_units, UR // 2, cols), F32),
            pltpu.VMEM((n_units, UR * 7 // 16, cols), F32),
            pltpu.VMEM((2, 8, cols), F32),
            pltpu.VMEM((rows_a, width), bf16),
            pltpu.VMEM((2, rows_a, 2 * UR), bf16),
            pltpu.VMEM((4, UR, cols), F32),
            pltpu.VMEM((SPOT_SLOTS, images, width), F32),
            pltpu.VMEM((SPOT_SLOTS, images, width), bf16),
        ] + [dma((n_units,)), dma((2 * LEVELS + 2, n_units)), dma((n_units,)), dma((2,)), dma((2, 2)), dma((SPOT_SLOTS,)), dma((SPOT_SLOTS,)), pltpu.SemaphoreType.REGULAR((LEVELS + 1, n_units))],
        compiler_params=pltpu.CompilerParams(collective_id=0, has_side_effects=True, vmem_limit_bytes=67043328),
        name='reduce_all',
    )(grad_fc, act, x_hat, short, gate, vec)


def forward_kernel(blocks, global_rows, a_ref, w_ref, s_ref, gamma_ref, beta_ref, lab_ref, bias_ref, wfc_ref, xh_ref, dfc_ref, gate_ref, vec_ref, wsq_ref, fsq_ref,
                   z0, z1, wb, stat, pool_s, cnt_s, sx_s, inv_s, big, fcb, sem):
    j = pl.program_id(0)
    spots, images, width = xh_ref.shape
    total = spots * images
    classes = wfc_ref.shape[0]
    load_fc = pltpu.make_async_copy(wfc_ref, big.at[pl.ds(0, classes)], sem.at[0])

    def run(now):
        w = w_ref[...]
        wb[...] = w.astype(jnp.bfloat16)
        wsq_ref[...] = jnp.sum((w * w).reshape(w.shape[0] // 8, 8, width), axis=0)
        out = jnp.dot(a_ref[...], wb[...], preferred_element_type=F32)
        now[...] = out.reshape(spots, images, width)
        mean = jnp.sum(out, axis=0, keepdims=True) / total
        d = out - mean
        var = jnp.sum(jnp.sum((d * d).reshape(total // 8, 8, width), axis=0), axis=0, keepdims=True) / total
        stat[0:1] = mean
        stat[1:2] = lax.rsqrt(var + BN_EPS)

    def finish(z):
        at = pl.ds(pl.multiple_of((j - 1) * width, 128), width)
        mean, inv = mean_inv
        gamma, beta = gamma_ref[:, at], beta_ref[:, at]
        inv_s[0:1, at] = inv
        zero = jnp.zeros((8, width), F32)
        for r in range(0, images, 8):
            img = pl.ds(r, 8)
            pool, cnt, sx = zero, zero, zero
            for p in range(spots):
                x = (z[p, img] - mean) * inv
                xh_ref[p, img] = x
                pre = x * gamma + beta + s_ref[p, img].astype(F32)
                on = pre > 0
                pool += jnp.where(on, pre, 0.0)
                cnt += jnp.where(on, 1.0, 0.0)
                sx += jnp.where(on, x, 0.0)
            pool_s[img, at], cnt_s[img, at], sx_s[img, at] = pool, cnt, sx

    mean_inv = stat[0:1], stat[1:2]
    pl.when(j == 0)(load_fc.start)

    @pl.when(j == 0)
    def _():
        run(z0)

    @pl.when(jnp.logical_and(jnp.logical_and(j > 0, j < blocks), j % 2 == 0))
    def _():
        run(z0)
        finish(z1)

    @pl.when(jnp.logical_and(j < blocks, j % 2 == 1))
    def _():
        run(z1)
        finish(z0)

    @pl.when(j == blocks)
    def _():
        finish(z1 if blocks % 2 == 0 else z0)
        load_fc.wait()
        spread = gamma_ref.shape[1]

        def pack(i, c):
            at = pl.ds(pl.multiple_of(i * 8, 8), 8)
            w = big[at]
            fcb[at] = w.astype(jnp.bfloat16)
            return c + w * w
        fsq_ref[...] = lax.fori_loop(0, classes // 8, pack, jnp.zeros((8, spread), F32))
        pooled = (pool_s[...] / spots).astype(jnp.bfloat16)
        wide = fcb[...]
        logits = lax.dot_general(pooled, wide, (((1,), (1,)), ((), ())), preferred_element_type=F32) + bias_ref[...]
        shifted = logits - jnp.max(logits, axis=1, keepdims=True)
        log_prob = shifted - jnp.log(jnp.sum(jnp.exp(shifted), axis=1, keepdims=True))
        square = (images, images)
        own = lax.broadcasted_iota(jnp.int32, square, 0) == lax.broadcasted_iota(jnp.int32, square, 1)
        labels = jnp.sum(jnp.where(own, lab_ref[...], 0), axis=1, keepdims=True)
        hit = labels == lax.broadcasted_iota(jnp.int32, logits.shape, 1)
        target = SMOOTHING / classes + (1.0 - SMOOTHING) * jnp.where(hit, 1.0, 0.0)
        loss = -jnp.sum(target * log_prob) / global_rows
        d_logits = (jnp.exp(log_prob) - target) / global_rows
        d_bias = jnp.sum(d_logits, axis=0, keepdims=True)
        d_bf = d_logits.astype(jnp.bfloat16)
        big[pl.ds(0, classes)] = lax.dot_general(d_bf, pooled, (((0,), (0,)), ((), ())), preferred_element_type=F32)
        d_pool = lax.dot_general(d_bf, wide, (((1,), (0,)), ((), ())), preferred_element_type=F32) / spots
        d_beta = jnp.sum(d_pool * cnt_s[...], axis=0, keepdims=True)
        d_gamma = jnp.sum(d_pool * sx_s[...], axis=0, keepdims=True)
        gi = gamma_ref[...] * inv_s[0:1]
        gate_ref[...] = d_pool * gi
        vec_ref[0:1] = gamma_ref[...]
        vec_ref[1:2] = beta_ref[...]
        vec_ref[2:3] = gi * (d_beta / total)
        vec_ref[3:4] = gi * (d_gamma / total)
        rest = big.shape[0] - classes
        big[pl.ds(classes, rest)] = jnp.zeros((rest, spread), F32)
        big[pl.ds(classes, 1)] = d_gamma
        big[pl.ds(classes + 1, 1)] = d_beta
        big[pl.ds(classes + 2, 1), pl.ds(0, classes)] = d_bias
        big[pl.ds(classes + 3, 1)] = jnp.full((1, spread), loss, F32)
        store = pltpu.make_async_copy(big, dfc_ref, sem.at[1])
        store.start()
        store.wait()


def forward(act, weight, short, gamma, beta, labels, bias, w_fct, global_rows):
    rows_a, c_mid = act.shape
    spots, images, c_out = short.shape
    classes = w_fct.shape[0]
    padded = -(-classes // (2 * UR)) * 2 * UR
    blocks = c_out // DB
    def now(j):
        return 0, jnp.minimum(j, blocks - 1)
    def late3(j):
        return 0, 0, jnp.maximum(j - 1, 0)
    def whole(shape):
        return pl.BlockSpec(shape, lambda j: (0,) * len(shape), pipeline_mode=pl.Buffered(1))
    hbm = pl.BlockSpec(memory_space=pl.ANY)
    rows8 = jax.ShapeDtypeStruct((8, c_out), F32)
    plane = pltpu.VMEM((images, c_out), F32)
    return pl.pallas_call(
        functools.partial(forward_kernel, blocks, global_rows),
        grid=(blocks + 1,),
        out_shape=(jax.ShapeDtypeStruct((spots, images, c_out), F32), jax.ShapeDtypeStruct((padded, c_out), F32),
                   jax.ShapeDtypeStruct((images, c_out), F32), rows8, rows8, rows8),
        in_specs=[whole((rows_a, c_mid)), pl.BlockSpec((c_mid, DB), now), pl.BlockSpec((spots, images, DB), late3),
                  whole(gamma.shape), whole(beta.shape), whole(labels.shape), whole(bias.shape), hbm],
        out_specs=(pl.BlockSpec((spots, images, DB), late3), hbm, pl.BlockSpec((images, c_out), lambda j: (0, 0)),
                   pl.BlockSpec((8, c_out), lambda j: (0, 0)), pl.BlockSpec((8, DB), now), pl.BlockSpec((8, c_out), lambda j: (0, 0))),
        scratch_shapes=[pltpu.VMEM((spots, images, DB), F32)] * 2 + [pltpu.VMEM((c_mid, DB), jnp.bfloat16), pltpu.VMEM((8, DB), F32),
                        plane, plane, plane, pltpu.VMEM((8, c_out), F32), pltpu.VMEM((padded, c_out), F32),
                        pltpu.VMEM((classes, c_out), jnp.bfloat16), pltpu.SemaphoreType.DMA((2,))],
        compiler_params=pltpu.CompilerParams(vmem_limit_bytes=63 * 2 ** 20),
        name='forward',
    )(act, weight, short, gamma, beta, labels, bias, w_fct)


def update_kernel(conv_steps, lr_ref, nrm_ref, csq_ref, fsq_ref, gc_ref, wc_ref, vc_ref, gf_ref, wf_ref, vf_ref,
                  small_ref, *refs):
    vectors, (wc_new, vc_new, wf_new, vf_new), vectors_new, (loss_ref, rate) = refs[:6], refs[6:10], refs[10:16], refs[16:]
    i = pl.program_id(0)
    lr = lr_ref[0, 0]

    @pl.when(i == 0)
    def _():
        for k, sq_ref in ((0, csq_ref), (1, fsq_ref)):
            w_norm = jnp.sqrt(jnp.sum(jnp.sum(sq_ref[...], axis=0, keepdims=True), axis=1, keepdims=True))
            g_norm = jnp.sqrt(jnp.sum(jnp.sum(nrm_ref[1 - k], axis=0, keepdims=True), axis=1, keepdims=True))
            rate[k:k + 1] = jnp.broadcast_to(lr * (TRUST_COEF * w_norm / (g_norm + WEIGHT_DECAY * w_norm)), (1, 128))

        for k in range(3):
            w_ref, v_ref = vectors[2 * k], vectors[2 * k + 1]
            v = MOMENTUM * v_ref[...] + lr * small_ref[k:k + 1, 0:w_ref.shape[1]]
            vectors_new[2 * k + 1][...] = v
            vectors_new[2 * k][...] = w_ref[...] - v
        loss_ref[...] = small_ref[3:4, 0:1]

    def apply(k, g_ref, w_ref, v_ref, w_out, v_out):
        scale = rate[k:k + 1, 0:1]

        def some(r, c):
            at = pl.ds(pl.multiple_of(r * 8, 8), 8)
            w = w_ref[at]
            v = MOMENTUM * v_ref[at] + scale * (g_ref[at] + WEIGHT_DECAY * w)
            v_out[at] = v
            w_out[at] = w - v
            return c
        lax.fori_loop(0, w_ref.shape[0] // 8, some, 0, unroll=True)

    pl.when(i < conv_steps)(lambda: apply(0, gc_ref, wc_ref, vc_ref, wc_new, vc_new))
    pl.when(i >= conv_steps)(lambda: apply(1, gf_ref, wf_ref, vf_ref, wf_new, vf_new))


def update(rate, norms, conv_sq, fc_sq, g_conv, w_conv, v_conv, g_fc, w_fct, v_fct, vectors):
    width = w_conv.shape[1]
    conv_rows, fc_rows = 256, 200
    conv_steps, fc_steps = w_conv.shape[0] // conv_rows, w_fct.shape[0] // fc_rows
    conv = pl.BlockSpec((conv_rows, width), lambda i: (jnp.minimum(i, conv_steps - 1), 0))
    fc = pl.BlockSpec((fc_rows, width), lambda i: (jnp.maximum(i - conv_steps, 0), 0))
    small = pl.BlockSpec((8, width), lambda i: (w_fct.shape[0] // 8, 0))
    vmem = pl.BlockSpec(memory_space=pltpu.VMEM)
    return pl.pallas_call(
        functools.partial(update_kernel, conv_steps),
        grid=(conv_steps + fc_steps,),
        out_shape=(jax.ShapeDtypeStruct(w_conv.shape, F32),) * 2 + (jax.ShapeDtypeStruct(w_fct.shape, F32),) * 2
        + tuple(jax.ShapeDtypeStruct(v.shape, F32) for v in vectors) + (jax.ShapeDtypeStruct((1, 1), F32),),
        in_specs=[pl.BlockSpec(memory_space=pltpu.SMEM), vmem, vmem, vmem, conv, conv, conv, fc, fc, fc, small] + [vmem] * 6,
        out_specs=(conv, conv, fc, fc) + (vmem,) * 7,
        scratch_shapes=[pltpu.VMEM((8, 128), F32)],
        compiler_params=pltpu.CompilerParams(vmem_limit_bytes=60 * 2 ** 20),
        name='update',
    )(rate, norms, conv_sq, fc_sq, g_conv, w_conv, v_conv, g_fc, w_fct, v_fct, g_fc, *vectors)


def solution(mesh):
    groups = mesh.shape['dp']

    def local_step(act_in, shortcut, labels, w_conv, bn_gamma, bn_beta, w_fc, fc_bias, vel_conv, vel_gamma, vel_beta, vel_fc, vel_bias, learn_rate):
        per_dev, side, _, c_mid = act_in.shape
        c_out = shortcut.shape[3]
        classes = w_fc.shape[1]
        spatial = side * side
        pos_count = per_dev * spatial
        global_rows = per_dev * groups
        act = act_in.transpose(1, 2, 0, 3).reshape(pos_count, c_mid)
        short = shortcut.transpose(1, 2, 0, 3).reshape(spatial, per_dev, c_out)
        x_hat, d_fc, gate, vec, conv_sq, fc_sq = forward(act, w_conv, short, bn_gamma[None], bn_beta[None], labels[None], fc_bias[None], w_fc.T, global_rows)
        g_fc, g_conv, norms = reduce_all(d_fc, act, x_hat, short, gate, vec, classes, groups)
        vectors = [v[None] for v in (bn_gamma, vel_gamma, bn_beta, vel_beta, fc_bias, vel_bias)]
        new = update(learn_rate[None, None], norms, conv_sq, fc_sq, g_conv, w_conv, vel_conv, g_fc, w_fc.T, vel_fc.T, vectors)
        conv_new, conv_vel, fc_new, fc_vel, gamma_new, gamma_vel, beta_new, beta_vel, bias_new, bias_vel, loss = new
        return (conv_new, gamma_new[0], beta_new[0], fc_new.T, bias_new[0], conv_vel, gamma_vel[0], beta_vel[0], fc_vel.T, bias_vel[0], loss[0, 0])

    return jax.shard_map(local_step, mesh=mesh, in_specs=(P('dp'),) * 3 + (P(),) * 11, out_specs=(P(),) * 11, check_vma=False)
```

```python
import functools

import jax
import jax.numpy as jnp
from jax import lax
from jax.experimental import pallas as pl
from jax.experimental.pallas import tpu as pltpu
from jax.sharding import PartitionSpec as P

BN_EPS = 1e-5
SMOOTHING = 0.1
MOMENTUM = 0.9
TRUST_COEF = 0.001
WEIGHT_DECAY = 5e-5

F32 = jnp.float32
UR = 128
CS = 2
OFFSETS = (0, 3, 5, 7, 9, 11, 13, 15, 18, 21)
SPOT_SLOTS = 4
DOT_COLS = 1024
DB = 256
PIECES = 7
LEVELS = 4
MESH_ID = pl.DeviceIdType.MESH


def bytes_wait(ref, sem):
    pltpu.make_async_copy(ref, ref, sem).wait()


def reduce_kernel(n_dev, fc_rows, fc_units, n_units, gf_ref, a_ref, xh_ref, s_ref, gp_ref, vec_ref, of_ref, oc_ref, nrm_ref,
                  g, ba, bm, acc, dz, abuf, stg, xbuf, sbuf,
                  ld, recv, send, osem, asem, xsem, ssem, credit):
    me = lax.axis_index('dp')
    core = me % 2
    partner = me + 1 - 2 * core
    cols = g.shape[2]
    size = [UR >> i for i in range(LEVELS + 1)]
    mine = pl.ds(pl.multiple_of(core * UR, 8), UR)
    other = pl.ds(pl.multiple_of((1 - core) * UR, 8), UR)

    def rows(off, size):
        return pl.ds(pl.multiple_of(off, 8), size)

    def remote(src, dst, u, k, dev):
        pltpu.make_async_remote_copy(src_ref=src, dst_ref=dst, send_sem=send.at[u], recv_sem=recv.at[k, u],
                                     device_id=(dev,), device_id_type=MESH_ID).start()

    def grant(k, u, dev):
        pl.semaphore_signal(credit.at[k, u], inc=1, device_id=(dev,), device_id_type=MESH_ID)

    def levels(u):
        s_a = 2 + 2 * (u % 2)
        keep = core * UR
        out = [(partner, keep, None)]
        for i, stride in enumerate((s_a, 8, 6 - s_a, 16), 1):
            bit = (me // stride) % 2
            give = keep + (1 - bit) * size[i]
            keep = keep + bit * size[i]
            out.append((me + stride * (1 - 2 * bit), keep, give))
        return out

    def landing(u, i):
        if i == 1:
            return ba.at[u]
        return bm.at[u, pl.ds(size[1] - size[i - 1], size[i])]

    barrier = pltpu.get_barrier_semaphore()

    def hello(d, c):
        pl.semaphore_signal(barrier, inc=1, device_id=((me + d) % n_dev,), device_id_type=MESH_ID)
        return c
    lax.fori_loop(1, n_dev, hello, 0)

    def hbm_slice(u, half):
        return rows((u // CS) * 2 * UR + half * UR, UR), pl.ds(pl.multiple_of((u % CS) * cols, 128), cols)

    def load_from(ref, first, last):
        def step(u, c):
            i, j = hbm_slice(u - first, core)
            pltpu.make_async_copy(ref.at[i, j], g.at[u, mine], ld.at[u]).start()
            return c
        lax.fori_loop(first, last, step, 0)

    def pair_from(ref, first, last):
        def step(u, c):
            i, j = hbm_slice(u - first, 1 - core)
            remote(ref.at[i, j], g.at[u, mine], u, 0, partner)
            return c
        lax.fori_loop(first, last, step, 0)

    spots, images = xh_ref.shape[0], xh_ref.shape[1]
    pieces = PIECES
    per_piece = spots // pieces
    assert per_piece * pieces == spots

    def fetch_spot(p):
        slot = p % SPOT_SLOTS
        pltpu.make_async_copy(xh_ref.at[p], xbuf.at[slot], xsem.at[slot]).start()
        pltpu.make_async_copy(s_ref.at[p], sbuf.at[slot], ssem.at[slot]).start()

    def fetch_a(k):
        for part, half in ((0, core), (1, 1 - core)):
            pltpu.make_async_copy(a_ref.at[:, pl.ds(pl.multiple_of(k * 2 * UR + half * UR, 128), UR)],
                                  abuf.at[k % 2, :, pl.ds(part * UR, UR)], asem.at[k % 2, part]).start()

    for p in range(SPOT_SLOTS):
        fetch_spot(p)
    load_from(gf_ref, 0, fc_units)
    fetch_a(0)
    fetch_a(1)
    acc[...] = jnp.zeros_like(acc)
    pl.semaphore_wait(barrier, n_dev - 1)
    pair_from(gf_ref, 0, fc_units)

    def spot_step(p, c):
        slot = p % SPOT_SLOTS
        bytes_wait(xbuf.at[slot], xsem.at[slot])
        bytes_wait(sbuf.at[slot], ssem.at[slot])

        def group(r, c):
            x = xbuf[slot, pl.ds(pl.multiple_of(r * 16, 16), 16)]
            pre = x * vec_ref[0:1] + vec_ref[1:2] + sbuf[slot, pl.ds(pl.multiple_of(r * 16, 16), 16)].astype(F32)
            d = jnp.where(pre > 0, gp_ref[pl.ds(pl.multiple_of(r * 16, 16), 16)], 0.0) - vec_ref[2:3] - x * vec_ref[3:4]
            dz[pl.ds(pl.multiple_of(p * images + r * 16, 16), 16)] = d.astype(jnp.bfloat16)
            return c
        lax.fori_loop(0, images // 16, group, 0)
        pl.when(p + SPOT_SLOTS < spots)(lambda: fetch_spot(p + SPOT_SLOTS))
        return c

    def weight_grad(u):
        v = u - fc_units
        k = v // CS
        cb = v % CS

        @pl.when(cb == 0)
        def _():
            for part in range(2):
                bytes_wait(abuf.at[k % 2, :, pl.ds(part * UR, UR)], asem.at[k % 2, part])

        def block(n, c):
            col = pl.multiple_of(n * DOT_COLS, 128)
            out = lax.dot_general(abuf[k % 2], dz[:, pl.ds(pl.multiple_of(cb * cols + col, 128), DOT_COLS)],
                                  (((0,), (0,)), ((), ())), preferred_element_type=F32)
            g[u, mine, pl.ds(col, DOT_COLS)] = out[:UR]
            stg[u % 4, :, pl.ds(col, DOT_COLS)] = out[UR:]
            return c
        lax.fori_loop(0, cols // DOT_COLS, block, 0)
        remote(stg.at[u % 4], g.at[u, mine], u, 0, partner)

        @pl.when(jnp.logical_and(cb == CS - 1, v + 1 + CS < n_units - fc_units))
        def _():
            fetch_a(k + 2)

    def reduce_stage(i, u):
        at = levels(u)
        dev, keep, _ = at[i]
        if i == 0:
            pl.when(u < fc_units)(lambda: bytes_wait(g.at[u, mine], ld.at[u]))
            bytes_wait(g.at[u, mine], send.at[u])
            bytes_wait(g.at[u, other], recv.at[0, u])
            g[u, mine] += g[u, other]
            grant(0, u, partner)
        else:
            bytes_wait(landing(u, i), send.at[u])
            grant(i, u, dev)
            bytes_wait(landing(u, i), recv.at[i, u])
            g[u, rows(keep, size[i])] += landing(u, i)[...]
        if i < LEVELS:
            dev, _, give = at[i + 1]
            remote(g.at[u, rows(give, size[i + 1])], landing(u, i + 1), u, i + 1, dev)
        else:
            gather_send(i, u, at)

    def gather_send(i, u, at):
        dev, keep, _ = at[i]
        pl.semaphore_wait(credit.at[i, u], 1)
        block = g.at[u, rows(keep, size[i])]
        remote(block, block, u, 2 * LEVELS + 1 - i, dev)

    def gather_stage(i, u):
        bytes_wait(landing(u, i), send.at[u])
        bytes_wait(landing(u, i), recv.at[2 * LEVELS + 1 - i, u])
        gather_send(i - 1, u, levels(u))

    def last_stage(u):
        bytes_wait(g.at[u, mine], send.at[u])
        bytes_wait(g.at[u, other], recv.at[2 * LEVELS + 1, u])
        is_fc = u < fc_units

        def out(ref, v, k):
            i, j = hbm_slice(v, 0)
            pltpu.make_async_copy(g.at[u], ref.at[rows((v // CS) * 2 * UR, 2 * UR), j], osem.at[k]).start()
        pl.when(is_fc)(lambda: out(of_ref, u, 0))
        pl.when(jnp.logical_not(is_fc))(lambda: out(oc_ref, u - fc_units, 1))
        kind = jnp.where(is_fc, 0, 1)
        limit = jnp.where(is_fc, fc_rows - (u // CS) * 2 * UR, 2 * UR)

        def square(k, c):
            x = g[u, rows(k * 8, 8)]
            return c + jnp.where(k * 8 < limit, x * x, 0.0)
        acc[kind] += lax.fori_loop(0, 2 * UR // 8, square, jnp.zeros((8, cols), F32))

    stages = ([functools.partial(reduce_stage, i) for i in range(LEVELS + 1)]
              + [functools.partial(gather_stage, i) for i in range(LEVELS, 0, -1)] + [last_stage])

    def step(t, c):
        for s in [*range(2 * LEVELS + 1, LEVELS, -1), *range(LEVELS, -1, -1)]:
            u = t - OFFSETS[s]
            pl.when(jnp.logical_and(u >= 0, u < n_units))(functools.partial(stages[s], u))

        @pl.when(t < pieces)
        def _():
            lax.fori_loop(t * per_piece, (t + 1) * per_piece, spot_step, 0)
        pl.when(jnp.logical_and(t + 1 >= fc_units, t + 1 < n_units))(lambda: weight_grad(t + 1))
        return c
    lax.fori_loop(0, n_units + OFFSETS[-1], step, 0)

    nrm_ref[...] = acc[...]
    bytes_wait(of_ref, osem.at[0])
    bytes_wait(oc_ref, osem.at[1])


def reduce_all(grad_fc, act, x_hat, short, gate, vec, fc_rows, n_dev):
    rows_a, c_mid = act.shape
    width = x_hat.shape[2]
    cols = width // CS
    fc_units = grad_fc.shape[0] // (2 * UR) * CS
    n_units = fc_units + c_mid // (2 * UR) * CS
    dma = pltpu.SemaphoreType.DMA
    hbm = pl.BlockSpec(memory_space=pl.ANY)
    vmem = pl.BlockSpec(memory_space=pltpu.VMEM)
    bf16 = jnp.bfloat16
    images = x_hat.shape[1]
    return pl.pallas_call(
        functools.partial(reduce_kernel, n_dev, fc_rows, fc_units, n_units),
        out_shape=(jax.ShapeDtypeStruct(grad_fc.shape, F32), jax.ShapeDtypeStruct((c_mid, width), F32),
                   jax.ShapeDtypeStruct((2, 8, cols), F32)),
        in_specs=[hbm, hbm, hbm, hbm, vmem, vmem],
        out_specs=(hbm, hbm, vmem),
        scratch_shapes=[
            pltpu.VMEM((n_units, 2 * UR, cols), F32),
            pltpu.VMEM((n_units, UR // 2, cols), F32),
            pltpu.VMEM((n_units, UR * 7 // 16, cols), F32),
            pltpu.VMEM((2, 8, cols), F32),
            pltpu.VMEM((rows_a, width), bf16),
            pltpu.VMEM((2, rows_a, 2 * UR), bf16),
            pltpu.VMEM((4, UR, cols), F32),
            pltpu.VMEM((SPOT_SLOTS, images, width), F32),
            pltpu.VMEM((SPOT_SLOTS, images, width), bf16),
        ] + [dma((n_units,)), dma((2 * LEVELS + 2, n_units)), dma((n_units,)), dma((2,)), dma((2, 2)), dma((SPOT_SLOTS,)), dma((SPOT_SLOTS,)), pltpu.SemaphoreType.REGULAR((LEVELS + 1, n_units))],
        compiler_params=pltpu.CompilerParams(collective_id=0, has_side_effects=True, vmem_limit_bytes=67043328),
        name='reduce_all',
    )(grad_fc, act, x_hat, short, gate, vec)


def forward_kernel(blocks, global_rows, a_ref, w_ref, s_ref, gamma_ref, beta_ref, lab_ref, bias_ref, wfc_ref, xh_ref, dfc_ref, gate_ref, vec_ref, wsq_ref, fsq_ref,
                   z0, z1, wb, stat, pool_s, cnt_s, sx_s, inv_s, big, fcb, sem):
    j = pl.program_id(0)
    spots, images, width = xh_ref.shape
    total = spots * images
    classes = wfc_ref.shape[0]
    load_fc = pltpu.make_async_copy(wfc_ref, big.at[pl.ds(0, classes)], sem.at[0])

    def run(now):
        w = w_ref[...]
        wb[...] = w.astype(jnp.bfloat16)
        wsq_ref[...] = jnp.sum((w * w).reshape(w.shape[0] // 8, 8, width), axis=0)
        out = jnp.dot(a_ref[...], wb[...], preferred_element_type=F32)
        now[...] = out.reshape(spots, images, width)
        mean = jnp.sum(out, axis=0, keepdims=True) / total
        d = out - mean
        var = jnp.sum(jnp.sum((d * d).reshape(total // 8, 8, width), axis=0), axis=0, keepdims=True) / total
        stat[0:1] = mean
        stat[1:2] = lax.rsqrt(var + BN_EPS)

    def finish(z):
        at = pl.ds(pl.multiple_of((j - 1) * width, 128), width)
        mean, inv = mean_inv
        gamma, beta = gamma_ref[:, at], beta_ref[:, at]
        inv_s[0:1, at] = inv
        zero = jnp.zeros((8, width), F32)
        for r in range(0, images, 8):
            img = pl.ds(r, 8)
            pool, cnt, sx = zero, zero, zero
            for p in range(spots):
                x = (z[p, img] - mean) * inv
                xh_ref[p, img] = x
                pre = x * gamma + beta + s_ref[p, img].astype(F32)
                on = pre > 0
                pool += jnp.where(on, pre, 0.0)
                cnt += jnp.where(on, 1.0, 0.0)
                sx += jnp.where(on, x, 0.0)
            pool_s[img, at], cnt_s[img, at], sx_s[img, at] = pool, cnt, sx

    mean_inv = stat[0:1], stat[1:2]
    pl.when(j == 0)(load_fc.start)

    @pl.when(j == 0)
    def _():
        run(z0)

    @pl.when(jnp.logical_and(jnp.logical_and(j > 0, j < blocks), j % 2 == 0))
    def _():
        run(z0)
        finish(z1)

    @pl.when(jnp.logical_and(j < blocks, j % 2 == 1))
    def _():
        run(z1)
        finish(z0)

    @pl.when(j == blocks)
    def _():
        finish(z1 if blocks % 2 == 0 else z0)
        load_fc.wait()
        spread = gamma_ref.shape[1]

        def pack(i, c):
            at = pl.ds(pl.multiple_of(i * 8, 8), 8)
            w = big[at]
            fcb[at] = w.astype(jnp.bfloat16)
            return c + w * w
        fsq_ref[...] = lax.fori_loop(0, classes // 8, pack, jnp.zeros((8, spread), F32))
        pooled = (pool_s[...] / spots).astype(jnp.bfloat16)
        wide = fcb[...]
        logits = lax.dot_general(pooled, wide, (((1,), (1,)), ((), ())), preferred_element_type=F32) + bias_ref[...]
        shifted = logits - jnp.max(logits, axis=1, keepdims=True)
        log_prob = shifted - jnp.log(jnp.sum(jnp.exp(shifted), axis=1, keepdims=True))
        square = (images, images)
        own = lax.broadcasted_iota(jnp.int32, square, 0) == lax.broadcasted_iota(jnp.int32, square, 1)
        labels = jnp.sum(jnp.where(own, lab_ref[...], 0), axis=1, keepdims=True)
        hit = labels == lax.broadcasted_iota(jnp.int32, logits.shape, 1)
        target = SMOOTHING / classes + (1.0 - SMOOTHING) * jnp.where(hit, 1.0, 0.0)
        loss = -jnp.sum(target * log_prob) / global_rows
        d_logits = (jnp.exp(log_prob) - target) / global_rows
        d_bias = jnp.sum(d_logits, axis=0, keepdims=True)
        d_bf = d_logits.astype(jnp.bfloat16)
        big[pl.ds(0, classes)] = lax.dot_general(d_bf, pooled, (((0,), (0,)), ((), ())), preferred_element_type=F32)
        d_pool = lax.dot_general(d_bf, wide, (((1,), (0,)), ((), ())), preferred_element_type=F32) / spots
        d_beta = jnp.sum(d_pool * cnt_s[...], axis=0, keepdims=True)
        d_gamma = jnp.sum(d_pool * sx_s[...], axis=0, keepdims=True)
        gi = gamma_ref[...] * inv_s[0:1]
        gate_ref[...] = d_pool * gi
        vec_ref[0:1] = gamma_ref[...]
        vec_ref[1:2] = beta_ref[...]
        vec_ref[2:3] = gi * (d_beta / total)
        vec_ref[3:4] = gi * (d_gamma / total)
        rest = big.shape[0] - classes
        big[pl.ds(classes, rest)] = jnp.zeros((rest, spread), F32)
        big[pl.ds(classes, 1)] = d_gamma
        big[pl.ds(classes + 1, 1)] = d_beta
        big[pl.ds(classes + 2, 1), pl.ds(0, classes)] = d_bias
        big[pl.ds(classes + 3, 1)] = jnp.full((1, spread), loss, F32)
        store = pltpu.make_async_copy(big, dfc_ref, sem.at[1])
        store.start()
        store.wait()


def forward(act, weight, short, gamma, beta, labels, bias, w_fct, global_rows):
    rows_a, c_mid = act.shape
    spots, images, c_out = short.shape
    classes = w_fct.shape[0]
    padded = -(-classes // (2 * UR)) * 2 * UR
    blocks = c_out // DB
    def now(j):
        return 0, jnp.minimum(j, blocks - 1)
    def late3(j):
        return 0, 0, jnp.maximum(j - 1, 0)
    def whole(shape):
        return pl.BlockSpec(shape, lambda j: (0,) * len(shape), pipeline_mode=pl.Buffered(1))
    hbm = pl.BlockSpec(memory_space=pl.ANY)
    rows8 = jax.ShapeDtypeStruct((8, c_out), F32)
    plane = pltpu.VMEM((images, c_out), F32)
    return pl.pallas_call(
        functools.partial(forward_kernel, blocks, global_rows),
        grid=(blocks + 1,),
        out_shape=(jax.ShapeDtypeStruct((spots, images, c_out), F32), jax.ShapeDtypeStruct((padded, c_out), F32),
                   jax.ShapeDtypeStruct((images, c_out), F32), rows8, rows8, rows8),
        in_specs=[whole((rows_a, c_mid)), pl.BlockSpec((c_mid, DB), now), pl.BlockSpec((spots, images, DB), late3),
                  whole(gamma.shape), whole(beta.shape), whole(labels.shape), whole(bias.shape), hbm],
        out_specs=(pl.BlockSpec((spots, images, DB), late3), hbm, pl.BlockSpec((images, c_out), lambda j: (0, 0)),
                   pl.BlockSpec((8, c_out), lambda j: (0, 0)), pl.BlockSpec((8, DB), now), pl.BlockSpec((8, c_out), lambda j: (0, 0))),
        scratch_shapes=[pltpu.VMEM((spots, images, DB), F32)] * 2 + [pltpu.VMEM((c_mid, DB), jnp.bfloat16), pltpu.VMEM((8, DB), F32),
                        plane, plane, plane, pltpu.VMEM((8, c_out), F32), pltpu.VMEM((padded, c_out), F32),
                        pltpu.VMEM((classes, c_out), jnp.bfloat16), pltpu.SemaphoreType.DMA((2,))],
        compiler_params=pltpu.CompilerParams(vmem_limit_bytes=63 * 2 ** 20),
        name='forward',
    )(act, weight, short, gamma, beta, labels, bias, w_fct)


def update_kernel(conv_steps, lr_ref, nrm_ref, csq_ref, fsq_ref, gc_ref, wc_ref, vc_ref, gf_ref, wf_ref, vf_ref,
                  small_ref, *refs):
    vectors, (wc_new, vc_new, wf_new, vf_new), vectors_new, (loss_ref, rate) = refs[:6], refs[6:10], refs[10:16], refs[16:]
    i = pl.program_id(0)
    lr = lr_ref[0, 0]

    @pl.when(i == 0)
    def _():
        for k, sq_ref in ((0, csq_ref), (1, fsq_ref)):
            w_norm = jnp.sqrt(jnp.sum(jnp.sum(sq_ref[...], axis=0, keepdims=True), axis=1, keepdims=True))
            g_norm = jnp.sqrt(jnp.sum(jnp.sum(nrm_ref[1 - k], axis=0, keepdims=True), axis=1, keepdims=True))
            rate[k:k + 1] = jnp.broadcast_to(lr * (TRUST_COEF * w_norm / (g_norm + WEIGHT_DECAY * w_norm)), (1, 128))

        for k in range(3):
            w_ref, v_ref = vectors[2 * k], vectors[2 * k + 1]
            v = MOMENTUM * v_ref[...] + lr * small_ref[k:k + 1, 0:w_ref.shape[1]]
            vectors_new[2 * k + 1][...] = v
            vectors_new[2 * k][...] = w_ref[...] - v
        loss_ref[...] = small_ref[3:4, 0:1]

    def apply(k, g_ref, w_ref, v_ref, w_out, v_out):
        scale = rate[k:k + 1, 0:1]

        def some(r, c):
            at = pl.ds(pl.multiple_of(r * 8, 8), 8)
            w = w_ref[at]
            v = MOMENTUM * v_ref[at] + scale * (g_ref[at] + WEIGHT_DECAY * w)
            v_out[at] = v
            w_out[at] = w - v
            return c
        lax.fori_loop(0, w_ref.shape[0] // 8, some, 0, unroll=True)

    pl.when(i < conv_steps)(lambda: apply(0, gc_ref, wc_ref, vc_ref, wc_new, vc_new))
    pl.when(i >= conv_steps)(lambda: apply(1, gf_ref, wf_ref, vf_ref, wf_new, vf_new))


def update(rate, norms, conv_sq, fc_sq, g_conv, w_conv, v_conv, g_fc, w_fct, v_fct, vectors):
    width = w_conv.shape[1]
    conv_rows, fc_rows = 256, 200
    conv_steps, fc_steps = w_conv.shape[0] // conv_rows, w_fct.shape[0] // fc_rows
    conv = pl.BlockSpec((conv_rows, width), lambda i: (jnp.minimum(i, conv_steps - 1), 0))
    fc = pl.BlockSpec((fc_rows, width), lambda i: (jnp.maximum(i - conv_steps, 0), 0))
    small = pl.BlockSpec((8, width), lambda i: (w_fct.shape[0] // 8, 0))
    vmem = pl.BlockSpec(memory_space=pltpu.VMEM)
    return pl.pallas_call(
        functools.partial(update_kernel, conv_steps),
        grid=(conv_steps + fc_steps,),
        out_shape=(jax.ShapeDtypeStruct(w_conv.shape, F32),) * 2 + (jax.ShapeDtypeStruct(w_fct.shape, F32),) * 2
        + tuple(jax.ShapeDtypeStruct(v.shape, F32) for v in vectors) + (jax.ShapeDtypeStruct((1, 1), F32),),
        in_specs=[pl.BlockSpec(memory_space=pltpu.SMEM), vmem, vmem, vmem, conv, conv, conv, fc, fc, fc, small] + [vmem] * 6,
        out_specs=(conv, conv, fc, fc) + (vmem,) * 7,
        scratch_shapes=[pltpu.VMEM((8, 128), F32)],
        compiler_params=pltpu.CompilerParams(vmem_limit_bytes=60 * 2 ** 20),
        name='update',
    )(rate, norms, conv_sq, fc_sq, g_conv, w_conv, v_conv, g_fc, w_fct, v_fct, g_fc, *vectors)


def solution(mesh):
    groups = mesh.shape['dp']

    def local_step(act_in, shortcut, labels, w_conv, bn_gamma, bn_beta, w_fc, fc_bias, vel_conv, vel_gamma, vel_beta, vel_fc, vel_bias, learn_rate):
        per_dev, side, _, c_mid = act_in.shape
        c_out = shortcut.shape[3]
        classes = w_fc.shape[1]
        spatial = side * side
        pos_count = per_dev * spatial
        global_rows = per_dev * groups
        act = act_in.transpose(1, 2, 0, 3).reshape(pos_count, c_mid)
        short = shortcut.transpose(1, 2, 0, 3).reshape(spatial, per_dev, c_out)
        x_hat, d_fc, gate, vec, conv_sq, fc_sq = forward(act, w_conv, short, bn_gamma[None], bn_beta[None], labels[None], fc_bias[None], w_fc.T, global_rows)
        g_fc, g_conv, norms = reduce_all(d_fc, act, x_hat, short, gate, vec, classes, groups)
        vectors = [v[None] for v in (bn_gamma, vel_gamma, bn_beta, vel_beta, fc_bias, vel_bias)]
        new = update(learn_rate[None, None], norms, conv_sq, fc_sq, g_conv, w_conv, vel_conv, g_fc, w_fc.T, vel_fc.T, vectors)
        conv_new, conv_vel, fc_new, fc_vel, gamma_new, gamma_vel, beta_new, beta_vel, bias_new, bias_vel, loss = new
        return (conv_new, gamma_new[0], beta_new[0], fc_new.T, bias_new[0], conv_vel, gamma_vel[0], beta_vel[0], fc_vel.T, bias_vel[0], loss[0, 0])

    return jax.shard_map(local_step, mesh=mesh, in_specs=(P('dp'),) * 3 + (P(),) * 11, out_specs=(P(),) * 11, check_vma=False)
```
